128 devices in a mesh: row: 16 (over y, z), col: 8 (over x, core).
Axes of the slice: x: 4, y: 4, z: 4, core: 2. Of those that a mesh axis runs over, the one named last changes fastest.
Arguments:
- densities: bfloat16 [18432, 3072], P(('row', 'col')), may hold values from -0.796875 to 0.796875
- counts: int32 [2048], P(('row', 'col')), may hold values from 3 to 9
- coulomb: float32 [3072], replicated, may hold values from 0.05 to 1
- energies: float32 [18432], P(('row', 'col')), may hold values from 8 to 64
- vectors: bfloat16 [18432, 64], P(('row', 'col')), may hold values from -0.046875 to 0.046875
Outputs:
- kernel: float32 [18432, 18432], P('row', 'col')
- product: float32 [18432, 64], P(('row', 'col'))
The draws below stay inside these ranges and needn't reach their ends.
All inputs are finite; a program needn't handle non-finite values.
Results may differ from the reference program's by a relative error of at most 0.0095.
Values may be sent and summed in bfloat16 or wider, within the bound.
A program may use at most 128 MiB of HBM per device.

```python
import math
import jax
import jax.numpy as jnp
from jax import lax

G = 3072
NV = 64
SLOT = 9
K_DEV = 16
NK = 2048
ROWS = 18432
N_ROW = 16
N_COL = 8


def set_ends(values, own_key, low, largest):
    spot = [jax.random.randint(jax.random.fold_in(own_key, axis), (), 0, length) for axis, length in enumerate(values.shape)]
    main_axis = values.shape.index(max(values.shape))
    beside = spot[:main_axis] + [(spot[main_axis] + 1) % values.shape[main_axis]] + spot[main_axis + 1:]
    return values.at[tuple(spot)].set(low).at[tuple(beside)].set(largest)


def levels(rng, shape, split, smallest, high):
    def one(position, shards_of):
        heights = jax.random.uniform(jax.random.fold_in(jax.random.fold_in(rng, 6), position), (shards_of,), jnp.float32, smallest / len(split), high / len(split))
        return jnp.repeat(jnp.exp(heights), shape[position] // shards_of).reshape((-1,) + (1,) * (len(shape) - position - 1))

    gain = one(*split[0])
    for cut in split[1:]:
        gain = gain * one(*cut)
    return gain


def noise(rng, dims, deviation, reach, shards=(), dtype=jnp.bfloat16):
    array = deviation * jax.random.normal(rng, dims, jnp.float32)
    if shards:
        array = array * levels(rng, dims, shards, -0.22, 0.18)
    return jnp.clip(array, -reach, reach).astype(dtype)


def setup_inputs(seed: int = 0) -> dict:
    seeds = jax.random.split(jax.random.key(seed), 6)
    densities = noise(seeds[0], (ROWS, G), 0.134, 0.796875, ((0, 128),))
    counts = set_ends(jax.random.randint(seeds[1], (NK,), 3, 10), jax.random.fold_in(seeds[1], 1), 3, 9).astype(jnp.int32)
    coulomb = jnp.clip(jnp.exp(jax.random.uniform(seeds[2], (G,), jnp.float32, math.log(0.05), math.log(1.0))), 0.05, 1.0)
    energies = jnp.clip(jnp.exp(math.log(64.0) - 2.0794415 * jax.random.uniform(seeds[3], (ROWS,), jnp.float32) ** levels(seeds[3], (ROWS,), ((0, 128),), -0.2, 0.2)), 8.0, 64.0)
    vectors = noise(seeds[4], (ROWS, NV), ROWS ** -0.5, 0.046875, ((0, 128),))
    return {"densities": densities, "counts": counts, "coulomb": coulomb, "energies": energies, "vectors": vectors}


def reference(densities, counts, coulomb, energies, vectors):
    slots_idx = lax.broadcasted_iota(jnp.int32, (NK, SLOT), 1)
    usable = (slots_idx < counts[:, None]).reshape(NK * SLOT)
    masked = jnp.where(usable[:, None], densities.astype(jnp.float32), 0.0)
    weighted = lax.optimization_barrier((masked * coulomb[None, :]).astype(jnp.bfloat16)).astype(jnp.float32)
    ordered = masked.reshape(N_ROW, N_COL, K_DEV * SLOT, G).transpose(1, 0, 2, 3).reshape(NK * SLOT, G)
    kernel = jnp.dot(weighted, ordered.T, precision=lax.Precision.HIGHEST, preferred_element_type=jnp.float32)
    projected = jnp.dot(masked.T, vectors.astype(jnp.float32), precision=lax.Precision.HIGHEST, preferred_element_type=jnp.float32)
    coupled = jnp.dot(weighted, projected, precision=lax.Precision.HIGHEST, preferred_element_type=jnp.float32)
    diagonal = jnp.where(usable, energies, 0.0)
    product = coupled + diagonal[:, None] * vectors.astype(jnp.float32)
    return kernel, product
```

```python
import functools

import jax
import jax.numpy as jnp
from jax import lax
from jax.experimental import pallas as pl
from jax.experimental.pallas import tpu as pltpu
from jax.sharding import PartitionSpec as P

MESH = pl.DeviceIdType.MESH
SLOT = 9
ROW_COL = ("row", "col")
NT = (((1,), (1,)), ((), ()))
DFS = (0, -1, 1, 2)
LAG2, LAG3, LAG4, LAGC = 1, 2, 3, 4
CHUNK = 256
COL_TILE = 768


def gather_kernel(
    dims,
    dens_ref,
    counts_ref,
    coul_ref,
    en_ref,
    vt_ref,
    acc,
    r_last,
    c_last,
    prod_ref,
    dn,
    wt,
    cbuf,
    rbuf,
    pb,
    rs1,
    qb,
    rs2,
    sb,
    rs3,
    tb,
    pf,
    in_sem,
    send_sem,
    recv_sem,
    psend,
    precv,
):
    blk, g_all, n_row, n_col = dims
    n = g_all // CHUNK
    nv = vt_ref.shape[0]
    half = CHUNK // 2
    row = lax.axis_index("row")
    col = lax.axis_index("col")
    core = col % 2
    first = (row // 4) * (1 - core) + (row % 4) * core
    second = (row % 4) * (1 - core) + (row // 4) * core

    def at(df, ds):
        f = (first + df + 4) % 4
        s = (second + ds + 4) % 4
        return f * (4 - 3 * core) + s * (1 + 3 * core)

    def xcol(dx, same=True):
        x = (col // 2 + dx + 4) % 4
        return 2 * x + (core if same else 1 - core)

    for g in range(n):
        lanes = slice(g * CHUNK, (g + 1) * CHUNK)
        pltpu.make_async_copy(dens_ref.at[:, lanes], dn.at[:, lanes], in_sem.at[g]).start()
    barrier = pltpu.get_barrier_semaphore()
    peers = [(row, (col + d) % n_col) for d in range(1, n_col)]
    peers += [(at(d, 0), col) for d in range(1, 4)] + [(at(0, d), col) for d in range(1, 4)]
    for peer in peers:
        pl.semaphore_signal(barrier, inc=1, device_id=peer, device_id_type=MESH)

    sub = lax.broadcasted_iota(jnp.int32, (blk, CHUNK), 0)
    lane = lax.broadcasted_iota(jnp.int32, (1, blk), 1)
    keep = sub < 0
    keep_lane = lane < 0
    for k in range(blk // SLOT):
        low, high = k * SLOT, k * SLOT + counts_ref[k]
        keep = keep | ((sub >= low) & (sub < high))
        keep_lane = keep_lane | ((lane >= low) & (lane < high))

    own_c = pl.multiple_of(row * blk, 16)
    own_r = pl.multiple_of(col * blk, 16)
    for g in range(n):
        lanes = slice(g * CHUNK, (g + 1) * CHUNK)
        pltpu.make_async_copy(dens_ref.at[:, lanes], dn.at[:, lanes], in_sem.at[g]).wait()
        masked = jnp.where(keep, dn[:, lanes].astype(jnp.float32), 0.0)
        weighted = (masked * coul_ref[:, lanes]).astype(jnp.bfloat16)
        masked = masked.astype(jnp.bfloat16)
        cbuf[g, pl.ds(own_c, blk), :] = masked
        rbuf[g, pl.ds(own_r, blk), :] = weighted
        dn[:, lanes] = masked
        wt[:, lanes] = weighted
    pl.semaphore_wait(barrier, len(peers))

    def copy(k, g, buf, block, part, peer):
        rows = pl.ds(pl.multiple_of(block * blk, 16), blk)
        lanes = {"all": pl.ds(0, CHUNK), "a": pl.ds(0, half), "b": pl.ds(half, half)}[part]
        ref = buf.at[g, rows, lanes]
        return pltpu.make_async_remote_copy(
            src_ref=ref,
            dst_ref=ref,
            send_sem=send_sem.at[g, k],
            recv_sem=recv_sem.at[g, k],
            device_id=peer,
            device_id_type=MESH,
        )

    fp, fm = (at(1, 0), col), (at(-1, 0), col)
    sp, sm = (at(0, 1), col), (at(0, -1), col)
    xp, xm = (row, xcol(1)), (row, xcol(-1))
    other = (row, xcol(0, False))
    kinds = [
        (cbuf, at(0, 0), "all", fp, at(-1, 0)),
        (cbuf, at(0, 0), "all", fm, at(1, 0)),
        (cbuf, at(-1, 0), "a", fp, at(2, 0)),
        (cbuf, at(1, 0), "b", fm, at(2, 0)),
    ]
    for df in DFS:
        kinds.append((cbuf, at(df, 0), "all", sp, at(df, -1)))
        kinds.append((cbuf, at(df, 0), "all", sm, at(df, 1)))
    for df in DFS:
        kinds.append((cbuf, at(df, -1), "a", sp, at(df, 2)))
        kinds.append((cbuf, at(df, 1), "b", sm, at(df, 2)))
    kinds += [
        (rbuf, xcol(0), "all", other, xcol(0, False)),
        (rbuf, xcol(0), "all", xp, xcol(-1)),
        (rbuf, xcol(0), "all", xm, xcol(1)),
        (rbuf, xcol(-1), "a", xp, xcol(2)),
        (rbuf, xcol(1), "b", xm, xcol(2)),
        (rbuf, xcol(-1), "all", other, xcol(-1, False)),
        (rbuf, xcol(1), "all", other, xcol(1, False)),
        (rbuf, xcol(2), "all", other, xcol(2, False)),
    ]

    def send(g, *ks):
        for k in ks:
            buf, block, part, peer, _ = kinds[k]
            copy(k, g, buf, block, part, peer).start()

    def got(g, *ks):
        for k in ks:
            buf, _, part, peer, block = kinds[k]
            copy(k, g, buf, block, part, peer).wait_recv()

    def stage1(g):
        send(g, 0, 1, 4, 5, 21, 22, 20)

    def stage2(g):
        got(g, 0)
        send(g, 2, 6, 7)
        got(g, 1)
        send(g, 3, 8, 9)
        got(g, 4)
        send(g, 12)
        got(g, 5)
        send(g, 13)
        got(g, 21)
        send(g, 23, 25)
        got(g, 22)
        send(g, 24, 26)

    def stage3(g):
        got(g, 2, 3)
        send(g, 10, 11)
        for k in (6, 7, 8, 9):
            got(g, k)
            send(g, k + 8)
        got(g, 23, 24)
        send(g, 27)

    def stage4(g):
        for k in (10, 11):
            got(g, k)
            send(g, k + 8)

    def arrived(g):
        got(g, 12, 13, 14, 15, 16, 17, 18, 19, 20, 25, 26, 27)

    def compute(g):
        @pl.loop(0, cbuf.shape[1] // COL_TILE)
        def _(j):
            lanes = pl.ds(pl.multiple_of(j * COL_TILE, COL_TILE), COL_TILE)
            acc[:, lanes] += lax.dot_general(
                rbuf[g], cbuf[g, lanes, :], NT, preferred_element_type=jnp.float32
            )

    width = g_all // n_col
    quarter = nv // 4

    def pcopy(k, src, dst, peer):
        return pltpu.make_async_remote_copy(
            src_ref=src,
            dst_ref=dst,
            send_sem=psend.at[k],
            recv_sem=precv.at[k],
            device_id=peer,
            device_id_type=MESH,
        )

    def to_cols(k0, src, dst, start):
        for d in range(1, n_col):
            to, frm = (col + d) % n_col, (col + n_col - d) % n_col
            slot = col if start else frm
            made = pcopy(k0 + d - 1, src(to), dst.at[slot], (row, to))
            if start:
                made.start()
            else:
                made.wait_recv()

    def ring_first(k0, src, dst, start):
        for d in range(1, 4):
            to = (first + d) % 4
            slot = first if start else (first + 4 - d) % 4
            made = pcopy(k0 + d - 1, src(to), dst.at[slot], (at(d, 0), col))
            if start:
                made.start()
            else:
                made.wait_recv()

    def ring_second(k0, src, dst, start):
        for d in range(1, 4):
            slot = second if start else (second + 4 - d) % 4
            made = pcopy(k0 + d - 1, src, dst.at[slot], (at(0, d), col))
            if start:
                made.start()
            else:
                made.wait_recv()

    def total(ref):
        value = ref[0].astype(jnp.float32)
        for i in range(1, ref.shape[0]):
            value = value + ref[i].astype(jnp.float32)
        return value

    def p_first():
        for i in range(n_col):
            part = jnp.dot(
                vt_ref[...], dn[:, i * width : (i + 1) * width], preferred_element_type=jnp.float32
            )
            pb[i] = part.astype(jnp.bfloat16)
        rs1[col] = pb[col]
        to_cols(0, lambda to: pb.at[to], rs1, True)

    def p_second():
        to_cols(0, lambda to: pb.at[to], rs1, False)
        value = total(rs1)
        for i in range(4):
            qb[i] = value[i * quarter : (i + 1) * quarter, :].astype(jnp.bfloat16)
        rs2[first] = qb[first]
        ring_first(7, lambda to: qb.at[to], rs2, True)

    def p_third():
        ring_first(7, lambda to: qb.at[to], rs2, False)
        value = total(rs2).astype(jnp.bfloat16)
        sb[...] = value
        rs3[second] = value
        ring_second(10, sb, rs3, True)

    def p_fourth():
        ring_second(10, sb, rs3, False)
        value = total(rs3).astype(jnp.bfloat16)
        sb2 = tb.at[first]
        sb2[...] = value
        ring_first(13, lambda to: tb.at[first], tb, True)

    def p_fifth():
        ring_first(13, lambda to: tb.at[first], tb, False)
        for i in range(4):
            pf[col, i * quarter : (i + 1) * quarter, :] = tb[i]
        to_cols(16, lambda to: pf.at[col], pf, True)

    def p_last():
        to_cols(16, lambda to: pf.at[col], pf, False)
        coupled = jnp.zeros((nv, blk), jnp.float32)
        for i in range(n_col):
            coupled = coupled + lax.dot_general(
                pf[i], wt[:, i * width : (i + 1) * width], NT, preferred_element_type=jnp.float32
            )
        diagonal = jnp.where(keep_lane, en_ref[...], 0.0)
        prod_ref[...] = coupled + diagonal * vt_ref[...].astype(jnp.float32)

    p_stages = (p_first, p_second, p_third, p_fourth, p_fifth, p_last)

    @pl.loop(0, n + LAG4)
    def _(t):
        def when(g, what):
            @pl.when((g >= 0) & (g < n))
            def _():
                what(g)

        when(t, stage1)
        when(t - LAG4, stage4)
        when(t - LAG3, stage3)
        when(t - LAG2, stage2)
        for i, stage in enumerate(p_stages):
            pl.when(t == i)(stage)

        @pl.when(t == 0)
        def _():
            @pl.loop(0, acc.shape[0] // 16)
            def _(i):
                rows = pl.ds(pl.multiple_of(i * 16, 16), 16)
                acc[rows, :] = jnp.zeros((16, acc.shape[1]), jnp.float32)

        @pl.when(t >= LAGC)
        def _():
            arrived(t - LAGC)
            compute(t - LAGC)

    for g in range(n + LAG4 - LAGC, n - 1):
        arrived(g)
        compute(g)
    arrived(n - 1)
    r_last[...] = rbuf[n - 1]
    c_last[...] = cbuf[n - 1]

    @pl.loop(0, n)
    def _(g):
        for k, (buf, block, part, peer, _) in enumerate(kinds):
            copy(k, g, buf, block, part, peer).wait_send()

    for d in range(1, n_col):
        to = (col + d) % n_col
        pcopy(d - 1, pb.at[to], rs1.at[col], (row, to)).wait_send()
        pcopy(15 + d, pf.at[col], pf.at[col], (row, to)).wait_send()
    for d in range(1, 4):
        to = (first + d) % 4
        pcopy(6 + d, qb.at[to], rs2.at[first], (at(d, 0), col)).wait_send()
        pcopy(9 + d, sb, rs3.at[second], (at(0, d), col)).wait_send()
        pcopy(12 + d, tb.at[first], tb.at[first], (at(d, 0), col)).wait_send()


def finish_kernel(acc, r_last, c_last, prod_in, out_ref, prod_out, stage, sem, psem):
    tile = stage.shape[2]
    steps = acc.shape[1] // tile
    product = pltpu.make_async_copy(prod_in, prod_out, psem)
    product.start()

    def out(j):
        return pltpu.make_async_copy(
            stage.at[j], out_ref.at[:, j * tile : (j + 1) * tile], sem.at[j]
        )

    for j in range(steps):
        lanes = slice(j * tile, (j + 1) * tile)
        stage[j] = acc[:, lanes] + lax.dot_general(
            r_last[...], c_last[lanes, :], NT, preferred_element_type=jnp.float32
        )
        out(j).start()
    for j in range(steps):
        out(j).wait()
    product.wait()


def solution(mesh):
    n_row, n_col = mesh.shape["row"], mesh.shape["col"]

    def body(densities, counts, coulomb, energies, vectors):
        blk, g_all = densities.shape
        nv = vectors.shape[1]
        n = g_all // CHUNK
        bf, f32 = jnp.bfloat16, jnp.float32
        rows, cols = n_col * blk, n_row * blk
        width = g_all // n_col
        dma = pltpu.SemaphoreType.DMA
        vmem = pl.BlockSpec(memory_space=pltpu.VMEM)
        acc, r_last, c_last, prod = pl.pallas_call(
            functools.partial(gather_kernel, (blk, g_all, n_row, n_col)),
            out_shape=(
                pltpu.VMEM((rows, cols), f32),
                pltpu.VMEM((rows, CHUNK), bf),
                pltpu.VMEM((cols, CHUNK), bf),
                pltpu.VMEM((nv, blk), f32),
            ),
            in_specs=[
                pl.BlockSpec(memory_space=pl.ANY),
                pl.BlockSpec(memory_space=pltpu.SMEM),
                vmem,
                vmem,
                vmem,
            ],
            out_specs=(vmem,) * 4,
            scratch_shapes=[
                pltpu.VMEM((blk, g_all), bf),
                pltpu.VMEM((blk, g_all), bf),
                pltpu.VMEM((n, cols, CHUNK), bf),
                pltpu.VMEM((n, rows, CHUNK), bf),
                pltpu.VMEM((n_col, nv, width), bf),
                pltpu.VMEM((n_col, nv, width), bf),
                pltpu.VMEM((4, nv // 4, width), bf),
                pltpu.VMEM((4, nv // 4, width), bf),
                pltpu.VMEM((nv // 4, width), bf),
                pltpu.VMEM((4, nv // 4, width), bf),
                pltpu.VMEM((4, nv // 4, width), bf),
                pltpu.VMEM((n_col, nv, width), bf),
                dma((n,)),
                dma((n, 28)),
                dma((n, 28)),
                dma((23,)),
                dma((23,)),
            ],
            compiler_params=pltpu.CompilerParams(
                collective_id=0, has_side_effects=True, vmem_limit_bytes=40 * 2**20
            ),
            name="gather",
        )(densities, counts, coulomb[None, :], energies[None, :], vectors.T)
        kernel, product = pl.pallas_call(
            finish_kernel,
            out_shape=(
                jax.ShapeDtypeStruct((rows, cols), f32),
                jax.ShapeDtypeStruct((nv, blk), f32),
            ),
            in_specs=[vmem] * 4,
            out_specs=(pl.BlockSpec(memory_space=pl.ANY),) * 2,
            scratch_shapes=[
                pltpu.VMEM((cols // CHUNK, rows, CHUNK), f32),
                dma((cols // CHUNK,)),
                dma,
            ],
            compiler_params=pltpu.CompilerParams(vmem_limit_bytes=40 * 2**20),
            name="finish",
        )(acc, r_last, c_last, prod)
        return kernel, product.T

    specs = (P(ROW_COL, None), P(ROW_COL), P(), P(ROW_COL), P(ROW_COL, None))
    return jax.shard_map(
        body,
        mesh=mesh,
        in_specs=specs,
        out_specs=(P("row", "col"), P(ROW_COL, None)),
        check_vma=False,
    )
```
